32 devices in a mesh: scen: 8 (over z, x), rootr: 2 (over core), rootc: 2 (over y).
Axes of the slice: x: 2, y: 2, z: 4, core: 2. Of those that a mesh axis runs over, the one named last changes fastest.
Arguments:
- start_guess: float32 [8192, 256], P(('scen', 'rootr'), 'rootc'), may hold values from -6 to 6
- right_side: float32 [8192, 256], P(('scen', 'rootr'), 'rootc'), may hold values from -6 to 6
- root_diagonal: float32 [8192], P(('scen', 'rootr')), may hold values from 1 to 4
- preconditioner: bfloat16 [8192, 8192], P(('scen', 'rootr')), may hold values from -0.015625 to 0.015625
- border_block: bfloat16 [16, 512, 768], P(('scen', 'rootr'), 'rootc'), may hold values from -0.21875 to 0.21875
- coupling_inverse: bfloat16 [16, 512, 512], P(('scen', 'rootr'), 'rootc'), may hold values from -0.25 to 0.25
- border_count: int32 [16], P(('scen', 'rootr')), may hold values from 64 to 512, as said below
- column_tiles: int32 [16, 6], P(('scen', 'rootr')), may hold values from 0 to 63, as said below
Outputs:
- final_iterate: float32 [8192, 256], P(('scen', 'rootr'), 'rootc')
The draws below stay inside these ranges and needn't reach their ends.
Inputs may be any that keep to these rules, and one draw needn't show every extreme that they name: A scenario's live border rows are its first border_count rows; some scenario has exactly 512. `column_tiles`: each row names 6 different tiles in rising order.
All inputs are finite; a program needn't handle non-finite values.
Results may differ from the reference program's by a relative error of at most 0.0022.
Values may be sent and summed in bfloat16 or wider, within the bound.
A program may use at most 64 MiB of HBM per device.

```python
import math
import jax
import jax.numpy as jnp
from jax import lax

ORDER = 8192
RHS = 256
BORDER = 512
TILE = 128
TOUCHED = 6
ITERS = 1
SCEN = 16
NTILES = 64
COUPLED = 768


def draw_border_count(key, part):
    first_key, second_key = jax.random.split(key)
    divisor = jax.random.randint(first_key, (SCEN,), 1, 9)
    counts = BORDER // divisor
    chosen = jax.random.randint(second_key, (), 0, SCEN)
    return jnp.where(jnp.arange(SCEN) == chosen, BORDER, counts).astype(jnp.int32)


def draw_column_tiles(key, part):
    scores = jax.random.randint(key, (SCEN, NTILES), 0, 1 << 20) * NTILES + jnp.arange(NTILES)[None, :]
    ordering = jnp.argsort(scores, axis=1)[:, :TOUCHED]
    return jnp.sort(ordering, axis=1).astype(jnp.int32)


def shard_levels(key, extent, pieces, least, largest):
    loudness, own = 1.0, jax.random.fold_in(key, 6)
    for position, parts in pieces:
        draws = jnp.exp(jax.random.uniform(jax.random.fold_in(own, position), (parts,), jnp.float32, least / len(pieces), largest / len(pieces)))
        loudness = loudness * jnp.repeat(draws, extent[position] // parts).reshape([-1 if axis == position else 1 for axis in range(len(extent))])
    return loudness


def centred(rng, extent, width, most, pieces=(), dtype=jnp.bfloat16):
    loudness = shard_levels(rng, extent, pieces, -0.22, 0.18) if pieces else 1.0
    values = jax.random.normal(rng, extent, jnp.float32) * width * loudness
    return jnp.minimum(jnp.maximum(values, -most), most).astype(dtype)


def setup_inputs(seed: int = 0) -> dict:
    seeds = jax.random.split(jax.random.key(seed), 9)
    start_guess = centred(seeds[0], (ORDER, RHS), 1.0, 6.0, ((0, 16), (1, 2)), jnp.float32)
    right_side = centred(seeds[1], (ORDER, RHS), 1.0, 6.0, ((0, 16), (1, 2)), jnp.float32)
    root_diagonal = jnp.clip(jnp.exp(math.log(4.0) - 1.3862944 * jax.random.uniform(seeds[2], (ORDER,), jnp.float32) ** shard_levels(seeds[2], (ORDER,), ((0, 16),), -0.2, 0.2)), 1.0, 4.0)
    preconditioner = centred(seeds[3], (ORDER, ORDER), (16 * ORDER) ** -0.5, 0.015625, ((0, 16),))
    border_block = centred(seeds[4], (SCEN, BORDER, COUPLED), COUPLED ** -0.5, 0.21875, ((0, 16), (1, 2)))
    coupling_inverse = centred(seeds[5], (SCEN, BORDER, BORDER), BORDER ** -0.5, 0.25, ((0, 16), (1, 2)))
    border_count = draw_border_count(jax.random.fold_in(seeds[8], 71), 0)
    column_tiles = draw_column_tiles(jax.random.fold_in(seeds[8], 71), 0)
    return {"start_guess": start_guess, "right_side": right_side, "root_diagonal": root_diagonal, "preconditioner": preconditioner, "border_block": border_block, "coupling_inverse": coupling_inverse, "border_count": border_count, "column_tiles": column_tiles}


def scenario_term(iterate_low, border, inverse_rows, live_count, tile_ids):
    picked = iterate_low.reshape(NTILES, TILE, RHS)[tile_ids].reshape(COUPLED, RHS)
    live_rows = (jnp.arange(BORDER) < live_count)[:, None]
    border_values = jnp.dot(border, picked, preferred_element_type=jnp.float32)
    border_values = jnp.where(live_rows, border_values, 0.0).astype(jnp.bfloat16)
    solved = jnp.dot(inverse_rows, border_values, preferred_element_type=jnp.float32)
    solved = jnp.where(live_rows, solved, 0.0).astype(jnp.bfloat16)
    return jnp.dot(border.T, solved, preferred_element_type=jnp.float32)


def reference(start_guess, right_side, root_diagonal, preconditioner, border_block, coupling_inverse, border_count, column_tiles):
    iterate = start_guess
    for iteration in range(ITERS):
        iterate_low = iterate.astype(jnp.bfloat16)

        def accumulate(running, scenario):
            border, inverse_rows, live_count, tile_ids = scenario
            term = scenario_term(iterate_low, border, inverse_rows, live_count, tile_ids)
            running = running.reshape(NTILES, TILE, RHS).at[tile_ids].add(term.reshape(TOUCHED, TILE, RHS))
            return running.reshape(ORDER, RHS), None

        coupling, unused = lax.scan(accumulate, jnp.zeros((ORDER, RHS), jnp.float32), (border_block, coupling_inverse, border_count, column_tiles))
        residual = right_side - root_diagonal[:, None] * iterate + coupling
        iterate = iterate + jnp.dot(preconditioner, residual.astype(jnp.bfloat16), preferred_element_type=jnp.float32)
    return iterate
```

```python
import functools
import math

import jax
import jax.numpy as jnp
from jax import lax
from jax.experimental import pallas as pl
from jax.experimental.pallas import tpu as pltpu
from jax.sharding import PartitionSpec as P

TILE = 128
CHUNKS = 2
MESH = pl.DeviceIdType.MESH


class Gather:
    def __init__(self, place, buf, rows, sems):
        chunks = min(CHUNKS, rows)
        self.place, self.buf, self.chunks = place, buf, chunks
        self.step = rows // chunks
        self.rows = rows
        self.ring_send, self.ring_recv, self.pair_send, self.pair_recv = sems
        self.sent = []

    def piece(self, scen, core, chunk):
        first = (scen * 2 + core) * self.rows + chunk * self.step
        return self.buf.at[pl.ds(first, self.step)]

    def slot(self, way, hop, chunk):
        return (way * (self.place.hops + 1) + hop) * self.chunks + chunk

    def carried(self, way, hop):
        if hop < self.place.hops:
            return range(self.chunks)
        return [way] if way < self.chunks else []

    def ring_copy(self, way, hop, chunk, scen):
        at = self.slot(way, hop, chunk)
        ref = self.piece(scen, self.place.core, chunk)
        return pltpu.make_async_remote_copy(
            src_ref=ref,
            dst_ref=ref,
            send_sem=self.ring_send.at[at],
            recv_sem=self.ring_recv.at[at],
            device_id={"scen": self.place.ahead[way]},
            device_id_type=MESH,
        )

    def pair_copy(self, way, hop, chunk, scen, core):
        at = self.slot(way, hop, chunk)
        ref = self.piece(scen, core, chunk)
        return pltpu.make_async_remote_copy(
            src_ref=ref,
            dst_ref=ref,
            send_sem=self.pair_send.at[at],
            recv_sem=self.pair_recv.at[at],
            device_id={"rootr": 1 - self.place.core},
            device_id_type=MESH,
        )

    def send(self, copy):
        copy.start()
        self.sent.append(copy)

    def begin(self):
        for chunk in range(self.chunks):
            for way in range(2):
                if chunk in self.carried(way, 1):
                    self.send(self.ring_copy(way, 1, chunk, self.place.scen))
        for chunk in range(self.chunks):
            self.send(self.pair_copy(0, 0, chunk, self.place.scen, self.place.core))

    def advance(self, hop):
        for chunk in range(self.chunks):
            for way in range(2):
                if chunk not in self.carried(way, hop):
                    continue
                scen = self.place.origin(way, hop)
                self.ring_copy(way, hop, chunk, scen).wait_recv()
                if hop < self.place.hops and chunk in self.carried(way, hop + 1):
                    self.send(self.ring_copy(way, hop + 1, chunk, scen))
                self.send(self.pair_copy(way, hop, chunk, scen, self.place.core))

    def settle(self, hop):
        for chunk in range(self.chunks):
            for way in range(2):
                if hop == 0:
                    if way == 0:
                        self.pair_copy(0, 0, chunk, self.place.scen, 1 - self.place.core).wait_recv()
                elif chunk in self.carried(way, hop):
                    scen = self.place.origin(way, hop)
                    self.pair_copy(way, hop, chunk, scen, 1 - self.place.core).wait_recv()

    def finish(self):
        for copy in self.sent:
            copy.wait_send()


class Place:
    def __init__(self, count):
        self.count, self.hops = count, count // 2
        self.scen, self.core = lax.axis_index("scen"), lax.axis_index("rootr")
        side, level = lax.rem(self.scen, 2), lax.div(self.scen, 2)
        self.spot = level * (1 - side) + (count - 1 - level) * side
        self.ahead = [self.at(1), self.at(count - 1)]

    def at(self, shift):
        spot = lax.rem(self.spot + shift, self.count)
        upper = lax.div(spot, self.hops)
        return (1 - upper) * 2 * spot + upper * (2 * (self.count - 1 - spot) + 1)

    def origin(self, way, hop):
        return self.at(self.count - hop if way == 0 else hop)

    def origin_traced(self, way, hop):
        return self.at(self.count - hop + way * (2 * hop - self.count))


def kernel(
    count,
    guess_ref,
    right_ref,
    diagonal_ref,
    precon_hbm,
    border_hbm,
    inverse_hbm,
    live_ref,
    own_tiles_ref,
    tiles_row_ref,
    out_ref,
    low_all,
    own_all,
    term_all,
    tiles_all,
    tiles_smem,
    precon,
    border,
    inverse,
    local_sems,
    precon_sems,
    cross_send,
    cross_recv,
    *ring_sems,
):
    place = Place(count)
    side = lax.axis_index("rootc")
    own_rows, half_rhs = guess_ref.shape
    half_rows, coupled = border_hbm.shape[1:]
    touched = coupled // TILE
    own_block = place.scen * 2 + place.core

    own_half = pl.ds(pl.multiple_of(side * half_rows, half_rows), half_rows)
    other_half = pl.ds(pl.multiple_of((1 - side) * half_rows, half_rows), half_rows)
    load_border = pltpu.make_async_copy(border_hbm.at[0], border.at[own_half], local_sems.at[0])
    load_inverse = pltpu.make_async_copy(inverse_hbm.at[0], inverse.at[own_half], local_sems.at[1])
    columns_count = precon.shape[0]

    def load_column(t):
        columns = pl.ds(pl.multiple_of(t * TILE, TILE), TILE)
        return pltpu.make_async_copy(precon_hbm.at[:, columns], precon.at[t], precon_sems.at[t])

    load_border.start()
    load_inverse.start()

    unit = low_all.shape[1]
    units = own_rows // unit
    per_tile = TILE // unit
    own_slice = pl.ds(own_block * units, units)
    split = (units, unit, half_rhs)
    low_all[own_slice] = guess_ref[...].astype(jnp.bfloat16).reshape(split)
    scale = jnp.broadcast_to(diagonal_ref[...], (half_rhs, own_rows)).T
    own_terms = right_ref[...] - scale * guess_ref[...]
    own_all[own_slice] = own_terms.astype(jnp.bfloat16).reshape(split)
    tiles_all[pl.ds(own_block, 1)] = tiles_row_ref[...]

    barrier = pltpu.get_barrier_semaphore()
    for peer in (
        {"scen": place.ahead[0]},
        {"scen": place.ahead[1]},
        {"rootr": 1 - place.core},
        {"rootc": 1 - side},
    ):
        pl.semaphore_signal(barrier, inc=1, device_id=peer, device_id_type=MESH)
    pl.semaphore_wait(barrier, 4)

    low = Gather(place, low_all, units, ring_sems[0:4])
    own = Gather(place, own_all, units, ring_sems[4:8])
    term = Gather(place, term_all, touched, ring_sems[8:12])
    tiles = Gather(place, tiles_all, 1, ring_sems[12:16])

    crossings = []
    low.begin()
    for index, (source, target) in enumerate(((border_hbm, border), (inverse_hbm, inverse))):
        crossing = pltpu.make_async_remote_copy(
            src_ref=source.at[0],
            dst_ref=target.at[own_half],
            send_sem=cross_send.at[index],
            recv_sem=cross_recv.at[index],
            device_id={"rootc": 1 - side},
            device_id_type=MESH,
        )
        crossing.start()
        crossings.append(crossing)
    tiles.begin()

    @pl.loop(0, columns_count)
    def start_column(t):
        load_column(t).start()

    for hop in range(1, place.hops + 1):
        low.advance(hop)
        tiles.advance(hop)
    own.begin()
    for hop in range(place.hops + 1):
        low.settle(hop)

    load_border.wait()
    crossings[0].wait_recv()
    live = jnp.clip(live_ref[0], 0, 2 * half_rows)
    live_mask = lax.broadcasted_iota(jnp.int32, (2 * half_rows, half_rhs), 0) < live
    picked = jnp.concatenate(
        [
            low_all[own_tiles_ref[0, k] * per_tile + part]
            for k in range(touched)
            for part in range(per_tile)
        ],
        axis=0,
    )
    values = jnp.dot(border[...], picked, preferred_element_type=jnp.float32)
    values = jnp.where(live_mask, values, 0.0).astype(jnp.bfloat16)
    load_inverse.wait()
    crossings[1].wait_recv()
    solved = jnp.dot(inverse[...], values, preferred_element_type=jnp.float32)
    solved = jnp.where(live_mask, solved, 0.0).astype(jnp.bfloat16)
    terms = lax.dot_general(
        border[...], solved, (((0,), (0,)), ((), ())), preferred_element_type=jnp.float32
    )
    term_all[pl.ds(own_block * touched, touched)] = terms.astype(jnp.bfloat16).reshape(
        touched, TILE, half_rhs
    )
    term.begin()

    for hop in range(place.hops + 1):
        tiles.settle(hop)
    to_smem = pltpu.make_async_copy(tiles_all, tiles_smem, local_sems.at[3])
    to_smem.start()
    to_smem.wait()

    @pl.loop(0, columns_count)
    def wait_column(t):
        load_column(t).wait()

    out_ref[...] = guess_ref[...]

    def product(columns, values, rows):
        left = jnp.concatenate([precon[t] for t in columns], axis=1)
        right = jnp.concatenate([values[t] for t in rows], axis=0)
        return jnp.dot(left, right, preferred_element_type=jnp.float32)

    def add_block(index, hop):
        way, core = lax.div(index, 2), lax.rem(index, 2)
        block = place.origin_traced(way, hop) * 2 + core
        total = jnp.zeros_like(out_ref)
        if own_rows % TILE == 0:
            own_tiles = own_rows // TILE
            for k in range(0, own_tiles, 2):
                group = [block * own_tiles + j for j in range(k, min(k + 2, own_tiles))]
                total = total + product(group, own_all, group)
        for k in range(0, touched, 2):
            group = range(k, min(k + 2, touched))
            total = total + product(
                [tiles_smem[block, 0, j] for j in group],
                term_all,
                [block * touched + j for j in group],
            )
        out_ref[...] += total

    def absorb(hop):
        own.settle(hop)
        term.settle(hop)
        ways = 1 if hop in (0, place.hops) else 2

        def body(index, carry):
            add_block(index, hop)
            return carry

        lax.fori_loop(0, 2 * ways, body, 0)

    for hop in range(1, place.hops + 1):
        own.advance(hop)
        term.advance(hop)
        absorb(hop - 1)
    absorb(place.hops)
    if own_rows % TILE != 0:

        @pl.loop(0, columns_count)
        def add_own(t):
            rows = [t * per_tile + part for part in range(per_tile)]
            out_ref[...] += product([t], own_all, rows)

    for gather in (low, own, term, tiles):
        gather.finish()
    for crossing in crossings:
        crossing.wait_send()


def local(
    count,
    start_guess,
    right_side,
    root_diagonal,
    preconditioner,
    border_block,
    coupling_inverse,
    border_count,
    column_tiles,
):
    own_rows, half_rhs = start_guess.shape
    order = preconditioner.shape[1]
    half_rows, coupled = border_block.shape[1:]
    blocks = count * 2
    touched = column_tiles.shape[1]
    tiles_row = jnp.pad(column_tiles, ((0, 0), (0, 128 - touched)))[:, None, :]
    hops = count // 2
    ring_sems = []
    unit = math.gcd(own_rows, TILE)
    units = own_rows // unit
    for rows in (units, units, touched, 1):
        chunks = min(CHUNKS, rows)
        ring_sems += [pltpu.SemaphoreType.DMA((2 * (hops + 1) * chunks,))] * 4
    vmem = pl.BlockSpec(memory_space=pltpu.VMEM)
    smem = pl.BlockSpec(memory_space=pltpu.SMEM)
    anywhere = pl.BlockSpec(memory_space=pltpu.HBM)
    return pl.pallas_call(
        functools.partial(kernel, count),
        out_shape=jax.ShapeDtypeStruct((own_rows, half_rhs), jnp.float32),
        in_specs=[vmem, vmem, vmem, anywhere, anywhere, anywhere, smem, smem, vmem],
        out_specs=vmem,
        scratch_shapes=[
            pltpu.VMEM((order // unit, unit, half_rhs), jnp.bfloat16),
            pltpu.VMEM((order // unit, unit, half_rhs), jnp.bfloat16),
            pltpu.VMEM((blocks * touched, TILE, half_rhs), jnp.bfloat16),
            pltpu.VMEM((blocks, 1, 128), jnp.int32),
            pltpu.SMEM((blocks, 1, 128), jnp.int32),
            pltpu.VMEM((order // TILE, own_rows, TILE), jnp.bfloat16),
            pltpu.VMEM((2 * half_rows, coupled), jnp.bfloat16),
            pltpu.VMEM((2 * half_rows, 2 * half_rows), jnp.bfloat16),
            pltpu.SemaphoreType.DMA((4,)),
            pltpu.SemaphoreType.DMA((order // TILE,)),
            pltpu.SemaphoreType.DMA((2,)),
            pltpu.SemaphoreType.DMA((2,)),
        ]
        + ring_sems,
        compiler_params=pltpu.CompilerParams(
            collective_id=0, has_side_effects=True, vmem_limit_bytes=60 * 1024 * 1024
        ),
    )(
        start_guess,
        right_side,
        root_diagonal[None, :],
        preconditioner,
        border_block,
        coupling_inverse,
        border_count,
        column_tiles,
        tiles_row,
    )


def solution(mesh):
    rows = ("scen", "rootr")
    placed = (
        P(rows, "rootc"),
        P(rows, "rootc"),
        P(rows),
        P(rows, None),
        P(rows, "rootc", None),
        P(rows, "rootc", None),
        P(rows),
        P(rows, None),
    )
    return jax.shard_map(
        functools.partial(local, mesh.shape["scen"]),
        mesh=mesh,
        in_specs=placed,
        out_specs=P(rows, "rootc"),
        check_vma=False,
    )
```

```python
import functools
import math

import jax
import jax.numpy as jnp
from jax import lax
from jax.experimental import pallas as pl
from jax.experimental.pallas import tpu as pltpu
from jax.sharding import PartitionSpec as P

TILE = 128
CHUNKS = 4
MESH = pl.DeviceIdType.MESH


class Gather:
    def __init__(self, place, buf, rows, sems):
        chunks = math.gcd(CHUNKS, rows)
        self.place, self.buf, self.chunks = place, buf, chunks
        self.step = rows // chunks
        self.rows = rows
        self.ring_send, self.ring_recv, self.pair_send, self.pair_recv = sems
        self.sent = []

    def piece(self, scen, core, chunk):
        first = (scen * 2 + core) * self.rows + chunk * self.step
        return self.buf.at[pl.ds(first, self.step)]

    def slot(self, way, hop, chunk):
        return (way * (self.place.hops + 1) + hop) * self.chunks + chunk

    def carried(self, way, hop):
        if hop < self.place.hops:
            return range(self.chunks)
        return [chunk for chunk in range(self.chunks) if chunk * 2 // self.chunks == way]

    def ring_copy(self, way, hop, chunk, scen):
        at = self.slot(way, hop, chunk)
        ref = self.piece(scen, self.place.core, chunk)
        return pltpu.make_async_remote_copy(
            src_ref=ref,
            dst_ref=ref,
            send_sem=self.ring_send.at[at],
            recv_sem=self.ring_recv.at[at],
            device_id={"scen": self.place.ahead[way]},
            device_id_type=MESH,
        )

    def pair_copy(self, way, hop, chunk, scen, core):
        at = self.slot(way, hop, chunk)
        ref = self.piece(scen, core, chunk)
        return pltpu.make_async_remote_copy(
            src_ref=ref,
            dst_ref=ref,
            send_sem=self.pair_send.at[at],
            recv_sem=self.pair_recv.at[at],
            device_id={"rootr": 1 - self.place.core},
            device_id_type=MESH,
        )

    def send(self, copy):
        copy.start()
        self.sent.append(copy)

    def begin(self, staggered=False):
        pending = []
        for chunk in range(self.chunks):
            if staggered:
                for copy in pending:
                    copy.wait_send()
                self.sent = [copy for copy in self.sent if all(copy is not p for p in pending)]
                pending = []
            for way in range(2):
                if chunk in self.carried(way, 1):
                    pending.append(self.ring_copy(way, 1, chunk, self.place.scen))
                    self.send(pending[-1])
        for chunk in range(self.chunks):
            self.send(self.pair_copy(0, 0, chunk, self.place.scen, self.place.core))

    def advance(self, hop):
        for chunk in range(self.chunks):
            for way in range(2):
                if chunk not in self.carried(way, hop):
                    continue
                scen = self.place.origin(way, hop)
                self.ring_copy(way, hop, chunk, scen).wait_recv()
                if hop < self.place.hops and chunk in self.carried(way, hop + 1):
                    self.send(self.ring_copy(way, hop + 1, chunk, scen))
                self.send(self.pair_copy(way, hop, chunk, scen, self.place.core))

    def settle(self, hop):
        for chunk in range(self.chunks):
            for way in range(2):
                if hop == 0:
                    if way == 0:
                        self.pair_copy(0, 0, chunk, self.place.scen, 1 - self.place.core).wait_recv()
                elif chunk in self.carried(way, hop):
                    scen = self.place.origin(way, hop)
                    self.pair_copy(way, hop, chunk, scen, 1 - self.place.core).wait_recv()

    def finish(self):
        for copy in self.sent:
            copy.wait_send()


class Place:
    def __init__(self, count):
        self.count, self.hops = count, count // 2
        self.scen, self.core = lax.axis_index("scen"), lax.axis_index("rootr")
        side, level = lax.rem(self.scen, 2), lax.div(self.scen, 2)
        self.spot = level * (1 - side) + (count - 1 - level) * side
        self.ahead = [self.at(1), self.at(count - 1)]

    def at(self, shift):
        spot = lax.rem(self.spot + shift, self.count)
        upper = lax.div(spot, self.hops)
        return (1 - upper) * 2 * spot + upper * (2 * (self.count - 1 - spot) + 1)

    def origin(self, way, hop):
        return self.at(self.count - hop if way == 0 else hop)

    def origin_traced(self, way, hop):
        return self.at(self.count - hop + way * (2 * hop - self.count))


def kernel(
    count,
    guess_ref,
    right_ref,
    diagonal_ref,
    precon_hbm,
    border_hbm,
    inverse_hbm,
    live_ref,
    own_tiles_ref,
    tiles_row_ref,
    out_ref,
    low_all,
    own_all,
    term_all,
    tiles_all,
    tiles_smem,
    precon,
    border,
    inverse,
    local_sems,
    precon_sems,
    cross_send,
    cross_recv,
    *ring_sems,
):
    place = Place(count)
    side = lax.axis_index("rootc")
    own_rows, half_rhs = guess_ref.shape
    half_rows, coupled = border_hbm.shape[1:]
    touched = coupled // TILE
    own_block = place.scen * 2 + place.core

    own_half = pl.ds(pl.multiple_of(side * half_rows, half_rows), half_rows)
    other_half = pl.ds(pl.multiple_of((1 - side) * half_rows, half_rows), half_rows)
    load_border = pltpu.make_async_copy(border_hbm.at[0], border.at[own_half], local_sems.at[0])
    load_inverse = pltpu.make_async_copy(inverse_hbm.at[0], inverse.at[own_half], local_sems.at[1])
    columns_count = precon.shape[0]

    def load_column(t):
        columns = pl.ds(pl.multiple_of(t * TILE, TILE), TILE)
        return pltpu.make_async_copy(precon_hbm.at[:, columns], precon.at[t], precon_sems.at[t])

    load_border.start()
    load_inverse.start()

    unit = low_all.shape[1]
    units = own_rows // unit
    per_tile = TILE // unit
    own_slice = pl.ds(own_block * units, units)
    split = (units, unit, half_rhs)
    low_all[own_slice] = guess_ref[...].astype(jnp.bfloat16).reshape(split)
    scale = jnp.broadcast_to(diagonal_ref[...], (half_rhs, own_rows)).T
    own_terms = right_ref[...] - scale * guess_ref[...]
    own_all[own_slice] = own_terms.astype(jnp.bfloat16).reshape(split)
    tiles_all[pl.ds(own_block, 1)] = tiles_row_ref[...]

    barrier = pltpu.get_barrier_semaphore()
    for peer in (
        {"scen": place.ahead[0]},
        {"scen": place.ahead[1]},
        {"rootr": 1 - place.core},
        {"rootc": 1 - side},
    ):
        pl.semaphore_signal(barrier, inc=1, device_id=peer, device_id_type=MESH)
    pl.semaphore_wait(barrier, 4)

    low = Gather(place, low_all, units, ring_sems[0:4])
    own = Gather(place, own_all, units, ring_sems[4:8])
    term = Gather(place, term_all, touched, ring_sems[8:12])
    tiles = Gather(place, tiles_all, 1, ring_sems[12:16])

    crossings = []
    low.begin(staggered=True)
    for index, (source, target) in enumerate(((border_hbm, border), (inverse_hbm, inverse))):
        crossing = pltpu.make_async_remote_copy(
            src_ref=source.at[0],
            dst_ref=target.at[own_half],
            send_sem=cross_send.at[index],
            recv_sem=cross_recv.at[index],
            device_id={"rootc": 1 - side},
            device_id_type=MESH,
        )
        crossing.start()
        crossings.append(crossing)
    tiles.begin()

    @pl.loop(0, columns_count)
    def start_column(t):
        load_column(t).start()

    for hop in range(1, place.hops + 1):
        low.advance(hop)
        tiles.advance(hop)
    own.begin()
    for hop in range(place.hops + 1):
        low.settle(hop)

    load_border.wait()
    crossings[0].wait_recv()
    live = jnp.clip(live_ref[0], 0, 2 * half_rows)
    live_mask = lax.broadcasted_iota(jnp.int32, (2 * half_rows, half_rhs), 0) < live
    picked = jnp.concatenate(
        [
            low_all[own_tiles_ref[0, k] * per_tile + part]
            for k in range(touched)
            for part in range(per_tile)
        ],
        axis=0,
    )
    values = jnp.dot(border[...], picked, preferred_element_type=jnp.float32)
    values = jnp.where(live_mask, values, 0.0).astype(jnp.bfloat16)
    load_inverse.wait()
    crossings[1].wait_recv()
    solved = jnp.dot(inverse[...], values, preferred_element_type=jnp.float32)
    solved = jnp.where(live_mask, solved, 0.0).astype(jnp.bfloat16)
    terms = lax.dot_general(
        border[...], solved, (((0,), (0,)), ((), ())), preferred_element_type=jnp.float32
    )
    term_all[pl.ds(own_block * touched, touched)] = terms.astype(jnp.bfloat16).reshape(
        touched, TILE, half_rhs
    )
    term.begin()

    for hop in range(place.hops + 1):
        tiles.settle(hop)
    to_smem = pltpu.make_async_copy(tiles_all, tiles_smem, local_sems.at[3])
    to_smem.start()
    to_smem.wait()

    @pl.loop(0, columns_count)
    def wait_column(t):
        load_column(t).wait()

    out_ref[...] = guess_ref[...]

    def product(columns, values, rows):
        left = jnp.concatenate([precon[t] for t in columns], axis=1)
        right = jnp.concatenate([values[t] for t in rows], axis=0)
        return jnp.dot(left, right, preferred_element_type=jnp.float32)

    def add_block(index, hop):
        way, core = lax.div(index, 2), lax.rem(index, 2)
        block = place.origin_traced(way, hop) * 2 + core
        total = jnp.zeros_like(out_ref)
        if own_rows % TILE == 0:
            own_tiles = own_rows // TILE
            for k in range(0, own_tiles, 2):
                group = [block * own_tiles + j for j in range(k, min(k + 2, own_tiles))]
                total = total + product(group, own_all, group)
        for k in range(0, touched, 2):
            group = range(k, min(k + 2, touched))
            total = total + product(
                [tiles_smem[block, 0, j] for j in group],
                term_all,
                [block * touched + j for j in group],
            )
        out_ref[...] += total

    def absorb(hop):
        own.settle(hop)
        term.settle(hop)
        ways = 1 if hop in (0, place.hops) else 2

        def body(index, carry):
            add_block(index, hop)
            return carry

        lax.fori_loop(0, 2 * ways, body, 0)

    for hop in range(1, place.hops + 1):
        own.advance(hop)
        term.advance(hop)
        absorb(hop - 1)
    absorb(place.hops)
    if own_rows % TILE != 0:

        @pl.loop(0, columns_count)
        def add_own(t):
            rows = [t * per_tile + part for part in range(per_tile)]
            out_ref[...] += product([t], own_all, rows)

    for gather in (low, own, term, tiles):
        gather.finish()
    for crossing in crossings:
        crossing.wait_send()


def local(
    count,
    start_guess,
    right_side,
    root_diagonal,
    preconditioner,
    border_block,
    coupling_inverse,
    border_count,
    column_tiles,
):
    own_rows, half_rhs = start_guess.shape
    order = preconditioner.shape[1]
    half_rows, coupled = border_block.shape[1:]
    blocks = count * 2
    touched = column_tiles.shape[1]
    tiles_row = jnp.pad(column_tiles, ((0, 0), (0, 128 - touched)))[:, None, :]
    hops = count // 2
    ring_sems = []
    unit = math.gcd(own_rows, TILE)
    units = own_rows // unit
    for rows in (units, units, touched, 1):
        chunks = math.gcd(CHUNKS, rows)
        ring_sems += [pltpu.SemaphoreType.DMA((2 * (hops + 1) * chunks,))] * 4
    vmem = pl.BlockSpec(memory_space=pltpu.VMEM)
    smem = pl.BlockSpec(memory_space=pltpu.SMEM)
    anywhere = pl.BlockSpec(memory_space=pltpu.HBM)
    return pl.pallas_call(
        functools.partial(kernel, count),
        out_shape=jax.ShapeDtypeStruct((own_rows, half_rhs), jnp.float32),
        in_specs=[vmem, vmem, vmem, anywhere, anywhere, anywhere, smem, smem, vmem],
        out_specs=vmem,
        scratch_shapes=[
            pltpu.VMEM((order // unit, unit, half_rhs), jnp.bfloat16),
            pltpu.VMEM((order // unit, unit, half_rhs), jnp.bfloat16),
            pltpu.VMEM((blocks * touched, TILE, half_rhs), jnp.bfloat16),
            pltpu.VMEM((blocks, 1, 128), jnp.int32),
            pltpu.SMEM((blocks, 1, 128), jnp.int32),
            pltpu.VMEM((order // TILE, own_rows, TILE), jnp.bfloat16),
            pltpu.VMEM((2 * half_rows, coupled), jnp.bfloat16),
            pltpu.VMEM((2 * half_rows, 2 * half_rows), jnp.bfloat16),
            pltpu.SemaphoreType.DMA((4,)),
            pltpu.SemaphoreType.DMA((order // TILE,)),
            pltpu.SemaphoreType.DMA((2,)),
            pltpu.SemaphoreType.DMA((2,)),
        ]
        + ring_sems,
        compiler_params=pltpu.CompilerParams(
            collective_id=0, has_side_effects=True, vmem_limit_bytes=60 * 1024 * 1024
        ),
    )(
        start_guess,
        right_side,
        root_diagonal[None, :],
        preconditioner,
        border_block,
        coupling_inverse,
        border_count,
        column_tiles,
        tiles_row,
    )


def solution(mesh):
    rows = ("scen", "rootr")
    placed = (
        P(rows, "rootc"),
        P(rows, "rootc"),
        P(rows),
        P(rows, None),
        P(rows, "rootc", None),
        P(rows, "rootc", None),
        P(rows),
        P(rows, None),
    )
    return jax.shard_map(
        functools.partial(local, mesh.shape["scen"]),
        mesh=mesh,
        in_specs=placed,
        out_specs=P(rows, "rootc"),
        check_vma=False,
    )
```
